32 devices in a mesh: grp: 4 (over y, x), row: 8 (over z, core).
Axes of the slice: x: 2, y: 2, z: 4, core: 2. Of those that a mesh axis runs over, the one named last changes fastest.
Arguments:
- owned_blocks: int32 [1024], P(('grp', 'row')), may hold values from 0 to 1023, as said below
- live_count: int32 [32], P(('grp', 'row')), may hold values from 9 to 36, as said below
- row_block: int32 [1152], P(('grp', 'row')), may hold values from 0 to 1023, as said below
- column_block: int32 [1152], P(('grp', 'row')), may hold values from 0 to 1023, as said below
- send_list: int32 [4, 8, 4, 24], P('grp', 'row'), may hold values from -1 to 31, as said below
- receive_list: int32 [4, 8, 4, 24], P('grp', 'row'), may hold values from -1 to 1023, as said below
- block_values: bfloat16 [1152, 256, 256], P(('grp', 'row')), as said below
- node_shift: float32 [1024, 256], P(('grp', 'row')), may hold values from 0.1 to 2
- start_vector: float32 [1024, 256], P(('grp', 'row')), as said below
Outputs:
- lanczos_basis: float32 [17, 1024, 256], P(None, ('grp', 'row'))
- tridiagonal: float32 [2, 16], replicated
The draws below stay inside these ranges and needn't reach their ends.
Inputs may be any that keep to these rules, and one draw needn't show every extreme that they name: `owned_blocks`: A permutation of the block ids 0 to 1023. `live_count`: some device has exactly 36 live slots in every draw. `row_block`: every slot's row block is owned by the slot's device. `column_block`: every slot's column block is owned by the slot's device or appears in that device's receive_list. Nonempty entries come first in each list and are distinct; a device sends nothing to itself; send_list[p, r, g] names exactly the blocks whose ids receive_list[g, r, p] lists, in the same order. Some list is full in every draw, and some device receives a full list from every peer. `receive_list`: matches send_list as stated there. `block_values`: entries are finite and of moderate size. `start_vector`: entries are finite and of order one.
All inputs are finite; a program needn't handle non-finite values.
Results may differ from the reference program's by a relative error of at most 0.0034.
Values may be sent and summed in bfloat16 or wider, within the bound.
A program may use at most 64 MiB of HBM per device.

```python
import math
import jax
import jax.numpy as jnp
from jax import lax

BLOCK = 256
BLOCKS_DEV = 32
STEPS = 16
SLOTS_DEV = 36
HALO = 24
BLOCKS = 1024
SLOTS = 1152
N_GRP = 4
N_ROW = 8


def layout(key):
    base = jax.random.fold_in(key, 9173)
    groups = N_GRP
    row_ranks = N_ROW
    devices_all = groups * row_ranks
    own_keys = jax.random.split(jax.random.fold_in(base, 1), row_ranks)
    shuffled = jax.vmap(lambda one_key: jax.random.permutation(one_key, groups * BLOCKS_DEV))(own_keys).astype(jnp.int32)
    owned_ids = jnp.arange(row_ranks, dtype=jnp.int32)[:, None] * (groups * BLOCKS_DEV) + shuffled
    owned_ids = owned_ids.reshape(row_ranks, groups, BLOCKS_DEV).transpose(1, 0, 2)
    sent_count = jax.random.randint(jax.random.fold_in(base, 2), (groups, groups, row_ranks), HALO // 4, HALO + 1)
    offset_peer = jax.random.randint(jax.random.fold_in(base, 3), (), 1, groups)
    sender_idx = jnp.arange(groups)[:, None, None]
    receiver_idx = jnp.arange(groups)[None, :, None]
    rank_idx = jnp.arange(row_ranks)[None, None, :]
    sent_count = jnp.where(sender_idx == (receiver_idx + offset_peer) % groups, HALO, sent_count)
    full_group = jax.random.randint(jax.random.fold_in(base, 4), (), 0, groups)
    full_rank = jax.random.randint(jax.random.fold_in(base, 5), (), 0, row_ranks)
    sent_count = jnp.where((receiver_idx == full_group) & (rank_idx == full_rank), HALO, sent_count)
    sent_count = jnp.where(sender_idx == receiver_idx, 0, sent_count)
    pick_keys = jax.random.split(jax.random.fold_in(base, 6), groups * groups * row_ranks)
    chosen = jax.vmap(lambda one_key: jax.random.permutation(one_key, BLOCKS_DEV))(pick_keys)
    chosen = chosen.reshape(groups, groups, row_ranks, BLOCKS_DEV)[..., :HALO].astype(jnp.int32)
    valid = jnp.arange(HALO)[None, None, None, :] < sent_count[..., None]
    send_full = jnp.where(valid, chosen, -1)
    owner_rows = jnp.broadcast_to(owned_ids[:, None, :, :], (groups, groups, row_ranks, BLOCKS_DEV))
    sent_ids = jnp.where(valid, jnp.take_along_axis(owner_rows, chosen, axis=3), -1)
    send_list = send_full.transpose(0, 2, 1, 3).astype(jnp.int32)
    receive_list = sent_ids.transpose(1, 2, 0, 3).astype(jnp.int32)
    owned_flat = owned_ids.reshape(devices_all, BLOCKS_DEV)
    spread = jax.random.randint(jax.random.fold_in(base, 7), (devices_all,), 0, 49)
    counts = jnp.maximum(SLOTS_DEV // 4, SLOTS_DEV * 16 // (16 + spread))
    busiest = jax.random.randint(jax.random.fold_in(base, 8), (), 0, devices_all)
    counts = jnp.where(jnp.arange(devices_all) == busiest, SLOTS_DEV, counts).astype(jnp.int32)
    first_rows = jax.vmap(lambda one_key: jax.random.permutation(one_key, BLOCKS_DEV))(jax.random.split(jax.random.fold_in(base, 9), devices_all))
    extra_rows = jax.random.randint(jax.random.fold_in(base, 10), (devices_all, SLOTS_DEV - BLOCKS_DEV), 0, BLOCKS_DEV)
    local_rows = jnp.concatenate([first_rows.astype(jnp.int32), extra_rows.astype(jnp.int32)], axis=1)
    row_ids = jnp.take_along_axis(owned_flat, local_rows, axis=1)
    pool = jnp.concatenate([owned_flat, receive_list.reshape(devices_all, groups * HALO)], axis=1)
    drawn = jax.random.randint(jax.random.fold_in(base, 11), (devices_all, SLOTS_DEV), 0, BLOCKS_DEV + groups * HALO)
    picked = jnp.take_along_axis(pool, drawn, axis=1)
    fallback = jnp.take_along_axis(owned_flat, drawn % BLOCKS_DEV, axis=1)
    column_ids = jnp.where(picked < 0, fallback, picked).astype(jnp.int32)
    return (owned_flat.reshape(-1), counts, row_ids.reshape(-1).astype(jnp.int32), column_ids.reshape(-1), send_list, receive_list)


def draw_owned_blocks(key, part):
    return layout(key)[0]


def draw_live_count(key, part):
    return layout(key)[1]


def draw_row_block(key, part):
    return layout(key)[2]


def draw_column_block(key, part):
    return layout(key)[3]


def draw_send_list(key, part):
    return layout(key)[4]


def draw_receive_list(key, part):
    return layout(key)[5]


def draw_block_values(key, part):
    device = (jnp.arange(SLOTS) // SLOTS_DEV).astype(jnp.float32)
    rising = 1.0 + 2.0 * device / max(N_GRP * N_ROW - 1, 1)
    samples = jax.random.normal(key, (SLOTS, BLOCK, BLOCK), jnp.float32)
    return (samples * (rising / BLOCK ** 0.5)[:, None, None]).astype(jnp.bfloat16)


def draw_start_vector(key, part):
    device = (jnp.arange(BLOCKS) // BLOCKS_DEV).astype(jnp.float32)
    rising = 1.0 + 2.0 * device / max(N_GRP * N_ROW - 1, 1)
    samples = jax.random.normal(key, (BLOCKS, BLOCK), jnp.float32)
    return (samples * rising[:, None]).astype(jnp.float32)


def steps_of(own_key, extent, cuts, least, top_value):
    def one(axis_at, blocks):
        draws = jax.random.uniform(jax.random.fold_in(jax.random.fold_in(own_key, 6), axis_at), (blocks,), jnp.float32, least / len(cuts), top_value / len(cuts))
        return jnp.repeat(jnp.exp(draws), extent[axis_at] // blocks).reshape((-1,) + (1,) * (len(extent) - axis_at - 1))

    loudness = one(*cuts[0])
    for cut in cuts[1:]:
        loudness = loudness * one(*cut)
    return loudness


def setup_inputs(seed: int = 0) -> dict:
    key_of = jax.random.split(jax.random.key(seed), 10)
    return {
        "owned_blocks": draw_owned_blocks(jax.random.fold_in(key_of[9], 71), 0),
        "live_count": draw_live_count(jax.random.fold_in(key_of[9], 71), 0),
        "row_block": draw_row_block(jax.random.fold_in(key_of[9], 71), 0),
        "column_block": draw_column_block(jax.random.fold_in(key_of[9], 71), 0),
        "send_list": draw_send_list(jax.random.fold_in(key_of[9], 71), 0),
        "receive_list": draw_receive_list(jax.random.fold_in(key_of[9], 71), 0),
        "block_values": draw_block_values(jax.random.fold_in(key_of[9], 71), 0),
        "node_shift": jnp.clip(jnp.exp(math.log(2.0) - 2.9957323 * jax.random.uniform(key_of[7], (BLOCKS, BLOCK), jnp.float32) ** steps_of(key_of[7], (BLOCKS, BLOCK), ((0, 32),), -0.2, 0.2)), 0.1, 2.0),
        "start_vector": draw_start_vector(jax.random.fold_in(key_of[9], 71), 0),
    }


def reference(owned_blocks, live_count, row_block, column_block, send_list, receive_list, block_values, node_shift, start_vector):
    groups = N_GRP
    row_ranks = N_ROW
    devices_all = groups * row_ranks
    owned_rows = owned_blocks.reshape(devices_all, BLOCKS_DEV)
    peer_base = (jnp.arange(groups, dtype=jnp.int32)[None, None, :, None] * row_ranks + jnp.arange(row_ranks, dtype=jnp.int32)[None, :, None, None]) * BLOCKS_DEV
    source_send = jnp.transpose(send_list, (2, 1, 0, 3))
    source_pos = (peer_base + jnp.clip(source_send, 0, BLOCKS_DEV - 1)).astype(jnp.int32).reshape(devices_all, groups * HALO)
    own_pos = jnp.arange(devices_all * BLOCKS_DEV, dtype=jnp.int32).reshape(devices_all, BLOCKS_DEV)
    known_ids = jnp.concatenate([owned_rows, receive_list.reshape(devices_all, groups * HALO)], axis=1)
    known_pos = jnp.concatenate([own_pos, source_pos], axis=1)
    columns_dev = column_block.reshape(devices_all, SLOTS_DEV)
    column_match = columns_dev[:, :, None] == known_ids[:, None, :]
    column_index = jnp.argmax(column_match.astype(jnp.int32), axis=2).astype(jnp.int32)
    column_pos = jnp.take_along_axis(known_pos, column_index, axis=1).reshape(-1)
    rows_dev = row_block.reshape(devices_all, SLOTS_DEV)
    row_match = rows_dev[:, :, None] == owned_rows[:, None, :]
    row_local = jnp.argmax(row_match.astype(jnp.int32), axis=2).astype(jnp.int32)
    row_pos = (own_pos[:, :1] + row_local).reshape(-1)
    keep_slot = jnp.arange(SLOTS_DEV, dtype=jnp.int32)[None, :] < live_count[:, None]
    weight = keep_slot.astype(jnp.float32).reshape(-1, 1)
    values_dev = block_values.reshape(devices_all, SLOTS_DEV, BLOCK, BLOCK)
    row_sums = lax.map(lambda part: lax.optimization_barrier(jnp.sum(part.astype(jnp.float32), axis=2)), values_dev).reshape(-1, BLOCK)
    degree = jax.ops.segment_sum(row_sums * weight, row_pos, num_segments=BLOCKS)
    diagonal = degree + node_shift

    def apply_operator(vector):
        rounded = vector.astype(jnp.bfloat16)
        gathered = rounded[column_pos].reshape(devices_all, SLOTS_DEV, BLOCK)
        products = lax.map(lambda pair: jnp.einsum('sab,sb->sa', pair[0].astype(jnp.float32), pair[1].astype(jnp.float32)), (values_dev, gathered)).reshape(-1, BLOCK)
        coupling = jax.ops.segment_sum(products * weight, row_pos, num_segments=BLOCKS)
        return diagonal * vector - coupling
    entries = BLOCKS * BLOCK
    highest = lax.Precision.HIGHEST
    first_vector = start_vector * lax.rsqrt(jnp.sum(start_vector * start_vector) / entries + 1e-06)
    krylov = jnp.zeros((STEPS + 1, BLOCKS, BLOCK), jnp.float32).at[0].set(first_vector)
    alphas = []
    betas = []
    for step_index in range(STEPS):
        applied = apply_operator(krylov[step_index])
        coefficient = jnp.einsum('kpb,pb->k', krylov, applied, precision=highest) / entries
        projected = applied - jnp.einsum('k,kpb->pb', coefficient, krylov, precision=highest)
        square_mean = jnp.sum(projected * projected) / entries
        alphas.append(coefficient[step_index])
        betas.append(jnp.sqrt(square_mean))
        krylov = krylov.at[step_index + 1].set(projected * lax.rsqrt(square_mean + 1e-06))
    tridiagonal = jnp.stack([jnp.stack(alphas), jnp.stack(betas)])
    return (krylov, tridiagonal)
```

```python
import functools

import jax
import jax.numpy as jnp
from jax import lax
from jax.experimental import pallas as pl
from jax.experimental.pallas import tpu as pltpu
from jax.sharding import PartitionSpec as P

STEPS = 16
LANES = 128
F32 = jnp.float32
BF16 = jnp.bfloat16
MESH = pl.DeviceIdType.MESH
NT = (((1,), (1,)), ((), ()))


def kernel(
    groups,
    ranks,
    owned_ref,
    live_ref,
    row_ref,
    column_ref,
    values_ref,
    shift_ref,
    start_ref,
    basis_ref,
    tri_ref,
    weights,
    mask,
    known,
    image,
    parts,
    ids,
    diagonal,
    weight_sem,
    image_send,
    image_recv,
    part_send,
    part_recv,
    id_send,
    id_recv,
):
    slots, block, _ = values_ref.shape
    rows = shift_ref.shape[0]
    devices = groups * ranks
    entries = float(devices * rows * block)
    my_group = lax.axis_index("grp")
    my_rank = lax.axis_index("row")
    me = my_group * ranks + my_rank
    packed_slots = -(-slots // 8) * 8

    def peer(group_step, rank_step):
        group = lax.rem(my_group + group_step, groups)
        rank = lax.rem(my_rank + rank_step, ranks)
        return group, rank

    offsets = [(g, r) for r in range(ranks - 1, -1, -1) for g in range(groups - 1, -1, -1)]
    offsets = [pair for pair in offsets if pair != (0, 0)]

    def each_other(action):
        if devices <= 64:
            for group_step, rank_step in offsets:
                action(*peer(group_step, rank_step))
        else:

            def body(at, carry):
                action(*peer(at // ranks, lax.rem(at, ranks)))
                return carry

            lax.fori_loop(1, devices, body, 0)

    weight_copy = pltpu.make_async_copy(values_ref, weights, weight_sem)
    weight_copy.start()

    barrier = pltpu.get_barrier_semaphore()
    each_other(
        lambda g, r: pl.semaphore_signal(barrier, inc=1, device_id=(g, r), device_id_type=MESH)
    )

    lane_row = lax.broadcasted_iota(jnp.int32, (1, LANES), 1)
    lane_tile = lax.broadcasted_iota(jnp.int32, (8, LANES), 1)
    wide = groups * rows
    wide_row = lax.broadcasted_iota(jnp.int32, (1, wide), 1)
    own_ids = jnp.zeros((1, wide), jnp.int32)
    own_column = jnp.zeros((rows, LANES), jnp.int32)
    row_iota = lax.broadcasted_iota(jnp.int32, (rows, LANES), 0)
    for at in range(rows):
        own_ids = jnp.where(lax.rem(wide_row, rows) == at, owned_ref[at], own_ids)
        own_column = jnp.where(row_iota == at, owned_ref[at], own_column)
    ids[0] = own_ids

    def part_sum(image_value, first):
        square = image_value * image_value
        tile = jnp.zeros((8, LANES), F32)

        def folded(product):
            total = None
            for top in range(0, rows, 8):
                for left in range(0, block, LANES):
                    piece = product[top : top + 8, left : left + LANES]
                    total = piece if total is None else total + piece
            return jnp.sum(total, axis=1, keepdims=True)

        tile = jnp.where(lane_tile == STEPS + 1, folded(square), tile)
        if not first:
            for k in range(STEPS):
                tile = jnp.where(lane_tile == k, folded(known[k, 0] * image_value), tile)
        return jnp.sum(tile, axis=0, keepdims=True)

    def image_copy(buffer, step):
        group, rank = peer(step, 0)
        return pltpu.make_async_remote_copy(
            src_ref=image.at[buffer, 0],
            dst_ref=image.at[buffer, groups - step],
            send_sem=image_send.at[buffer, step],
            recv_sem=image_recv.at[buffer, groups - step],
            device_id=(group, rank),
            device_id_type=MESH,
        )

    def image_wait(buffer, step):
        pltpu.make_async_copy(
            image.at[buffer, step], image.at[buffer, step], image_recv.at[buffer, step]
        ).wait()

    def part_start(buffer):
        def send(group, rank):
            pltpu.make_async_remote_copy(
                src_ref=parts.at[buffer, me],
                dst_ref=parts.at[buffer, me],
                send_sem=part_send.at[buffer],
                recv_sem=part_recv.at[buffer],
                device_id=(group, rank),
                device_id_type=MESH,
            ).start()

        each_other(send)

    def part_wait(buffer, sem):
        others = parts.at[buffer, pl.ds(0, devices - 1)]
        pltpu.make_async_copy(others, others, sem.at[buffer]).wait()

    def id_copy(step):
        group, rank = peer(step, 0)
        return pltpu.make_async_remote_copy(
            src_ref=ids.at[0],
            dst_ref=ids.at[groups - step],
            send_sem=id_send.at[step],
            recv_sem=id_recv.at[groups - step],
            device_id=(group, rank),
            device_id_type=MESH,
        )

    def totals(buffer):
        total = parts[buffer, 0]
        for at in range(1, devices):
            total = total + parts[buffer, at]
        total = total * (1.0 / entries)
        signed = jnp.where(lane_row <= STEPS, -total * total, 0.0)
        signed = jnp.where(lane_row == STEPS + 1, total, signed)
        square_mean = jnp.sum(signed, axis=1, keepdims=True)
        return total, square_mean

    start = start_ref[...]
    image[0, 0] = start
    parts[0, me] = part_sum(start, True)

    pl.semaphore_wait(barrier, devices - 1)
    for step in range(1, groups):
        id_copy(step).start()
    part_start(0)
    for step in range(1, groups):
        image_copy(0, step).start()

    known[...] = jnp.zeros_like(known)
    for s in range(slots):
        row = jnp.where(s < live_ref[0], row_ref[s], -1)
        mask[s] = (own_column == row).astype(F32).astype(BF16)
    column = jnp.full((packed_slots, wide), -1, jnp.int32)
    slot_iota = lax.broadcasted_iota(jnp.int32, (packed_slots, wide), 0)
    for s in range(slots):
        column = jnp.where(slot_iota == s, column_ref[s], column)

    weight_copy.wait()
    degree = jnp.zeros((rows, block), F32)
    for s in range(slots):
        lhs = jnp.concatenate([mask[s]] * (block // LANES), axis=1)
        degree = degree + lax.dot_general(lhs, weights[s], NT, preferred_element_type=F32)
    diagonal[...] = degree + shift_ref[...]

    for step in range(1, groups):
        id_copy(step).wait_send()
    for step in range(1, groups):
        pltpu.make_async_copy(ids.at[step], ids.at[step], id_recv.at[step]).wait()
    known_ids = ids[0]
    for step in range(1, groups):
        known_ids = jnp.where(wide_row // rows == step, ids[step], known_ids)
    gather = (column == known_ids).astype(F32).astype(BF16)

    def spread(total, square_mean):
        scale = jnp.broadcast_to(lax.rsqrt(square_mean + 1e-06), (8, LANES))
        tile = jnp.broadcast_to(total, (8, LANES))
        coefficients = [
            jnp.broadcast_to(tile[:, k : k + 1], (8, LANES)) for k in range(STEPS)
        ]
        return coefficients, scale

    def orthogonal(buffer, step, coefficients, scale):
        pieces = []
        for top in range(0, rows, 8):
            line = []
            for left in range(0, block, LANES):
                at = (pl.ds(top, 8), pl.ds(left, LANES))
                value = image[(buffer, step) + at]
                for k in range(STEPS):
                    value = value - coefficients[k] * known[(k, step) + at]
                line.append(value * scale)
            pieces.append(jnp.concatenate(line, axis=1))
        return jnp.concatenate(pieces, axis=0)

    def record(it, total, square_mean, alpha, beta):
        here = lane_row == it - 1
        alpha = jnp.where(here, total, alpha)
        beta = jnp.where(here, jnp.sqrt(square_mean), beta)
        return alpha, beta

    def body(it, state):
        alpha, beta = state
        now = lax.rem(it, 2)
        later = 1 - now
        part_wait(now, part_recv)
        total, square_mean = totals(now)
        alpha, beta = record(it, total, square_mean, alpha, beta)
        coefficients, scale = spread(total, square_mean)
        vectors = []
        for step in range(groups):
            if step:
                image_wait(now, step)
            vector = orthogonal(now, step, coefficients, scale)
            known[it, step] = vector
            if step == 0:
                basis_ref[it] = vector
            vectors.append(vector.astype(BF16))
        gathered = jnp.dot(
            gather, jnp.concatenate(vectors, axis=0), preferred_element_type=F32
        )
        coupling = jnp.zeros((rows, block), F32)
        for s in range(slots):
            line = jnp.broadcast_to(gathered[s : s + 1], (rows, block)).astype(BF16)
            lhs = line * jnp.concatenate([mask[s]] * (block // LANES), axis=1)
            coupling = coupling + lax.dot_general(
                lhs, weights[s], NT, preferred_element_type=F32
            )
        applied = diagonal[...] * known[it, 0] - coupling

        part_wait(now, part_send)
        for step in range(1, groups):
            image_copy(now, step).wait_send()
        image[later, 0] = applied
        parts[later, me] = part_sum(applied, False)
        part_start(later)

        @pl.when(it < STEPS - 1)
        def _():
            for step in range(1, groups):
                image_copy(later, step).start()

        return alpha, beta

    zero = jnp.zeros((1, LANES), F32)
    alpha, beta = lax.fori_loop(0, STEPS, body, (zero, zero))
    last = STEPS % 2
    part_wait(last, part_recv)
    part_wait(last, part_send)
    total, square_mean = totals(last)
    alpha, beta = record(STEPS, total, square_mean, alpha, beta)
    coefficients, scale = spread(total, square_mean)
    basis_ref[STEPS] = orthogonal(last, 0, coefficients, scale)
    tri_ref[...] = jnp.concatenate([alpha[:, :STEPS], beta[:, :STEPS]], axis=0)


def shards(
    owned_blocks,
    live_count,
    row_block,
    column_block,
    send_list,
    receive_list,
    block_values,
    node_shift,
    start_vector,
):
    rows, block = start_vector.shape
    slots = block_values.shape[0]
    groups = lax.axis_size("grp")
    ranks = lax.axis_size("row")
    devices = groups * ranks
    smem = pl.BlockSpec(memory_space=pltpu.SMEM)
    vmem = pl.BlockSpec(memory_space=pltpu.VMEM)
    dma = pltpu.SemaphoreType.DMA
    return pl.pallas_call(
        functools.partial(kernel, groups, ranks),
        out_shape=(
            jax.ShapeDtypeStruct((STEPS + 1, rows, block), F32),
            jax.ShapeDtypeStruct((2, STEPS), F32),
        ),
        in_specs=[smem, smem, smem, smem, pl.BlockSpec(memory_space=pl.ANY), vmem, vmem],
        out_specs=(vmem, vmem),
        scratch_shapes=[
            pltpu.VMEM((slots, block, block), BF16),
            pltpu.VMEM((slots, rows, LANES), BF16),
            pltpu.VMEM((STEPS, groups, rows, block), F32),
            pltpu.VMEM((2, groups, rows, block), F32),
            pltpu.VMEM((2, devices, 1, LANES), F32),
            pltpu.VMEM((groups, 1, groups * rows), jnp.int32),
            pltpu.VMEM((rows, block), F32),
            dma,
            dma((2, groups)),
            dma((2, groups)),
            dma((2,)),
            dma((2,)),
            dma((groups,)),
            dma((groups,)),
        ],
        compiler_params=pltpu.CompilerParams(
            collective_id=0, has_side_effects=True, vmem_limit_bytes=48 * 1024 * 1024
        ),
    )(owned_blocks, live_count, row_block, column_block, block_values, node_shift, start_vector)


def solution(mesh):
    return jax.shard_map(
        shards,
        mesh=mesh,
        in_specs=(
            P(("grp", "row")),
            P(("grp", "row")),
            P(("grp", "row")),
            P(("grp", "row")),
            P("grp", "row", None, None),
            P("grp", "row", None, None),
            P(("grp", "row"), None, None),
            P(("grp", "row"), None),
            P(("grp", "row"), None),
        ),
        out_specs=(P(None, ("grp", "row"), None), P()),
        check_vma=False,
    )
```

```python
import functools

import jax
import jax.numpy as jnp
from jax import lax
from jax.experimental import pallas as pl
from jax.experimental.pallas import tpu as pltpu
from jax.sharding import PartitionSpec as P

STEPS = 16
LANES = 128
F32 = jnp.float32
BF16 = jnp.bfloat16
MESH = pl.DeviceIdType.MESH
NT = (((1,), (1,)), ((), ()))


SQUARES = STEPS + 1
SHIFT = STEPS + 2


def tree(terms):
    while len(terms) > 1:
        pairs = [terms[at] + terms[at + 1] for at in range(0, len(terms) - 1, 2)]
        terms = pairs + terms[len(pairs) * 2 :]
    return terms[0]


def kernel(
    groups,
    ranks,
    owned_ref,
    live_ref,
    row_ref,
    column_ref,
    values_ref,
    shift_ref,
    start_ref,
    basis_ref,
    tri_ref,
    weights,
    mask,
    known,
    mapped,
    image,
    parts,
    ids,
    diagonal,
    weight_sem,
    image_send,
    image_recv,
    part_send,
    part_recv,
    id_send,
    id_recv,
):
    slots, block, _ = values_ref.shape
    rows = shift_ref.shape[0]
    devices = groups * ranks
    entries = float(devices * rows * block)
    my_group = lax.axis_index("grp")
    my_rank = lax.axis_index("row")
    me = my_group * ranks + my_rank
    packed_slots = -(-slots // 8) * 8

    def wrapped(value, size):
        return jnp.where(value >= size, value - size, value)

    if devices <= 64:
        group_at = [wrapped(my_group + step, groups) for step in range(groups)]
        rank_at = [wrapped(my_rank + step, ranks) for step in range(ranks)]

        def peer(group_step, rank_step):
            return group_at[group_step], rank_at[rank_step]

    else:

        def peer(group_step, rank_step):
            return (
                wrapped(my_group + group_step, groups),
                wrapped(my_rank + rank_step, ranks),
            )

    offsets = [(g, r) for r in range(ranks - 1, -1, -1) for g in range(groups - 1, -1, -1)]
    offsets = [pair for pair in offsets if pair != (0, 0)]

    def each_other(action):
        if devices <= 64:
            for group_step, rank_step in offsets:
                action(*peer(group_step, rank_step))
        else:

            def body(at, carry):
                action(*peer(at // ranks, lax.rem(at, ranks)))
                return carry

            lax.fori_loop(1, devices, body, 0)

    weight_copy = pltpu.make_async_copy(values_ref, weights, weight_sem)
    weight_copy.start()

    barrier = pltpu.get_barrier_semaphore()
    each_other(
        lambda g, r: pl.semaphore_signal(barrier, inc=1, device_id=(g, r), device_id_type=MESH)
    )

    lane_row = lax.broadcasted_iota(jnp.int32, (1, LANES), 1)
    lane_tile = lax.broadcasted_iota(jnp.int32, (8, LANES), 1)
    wide = groups * rows
    wide_row = lax.broadcasted_iota(jnp.int32, (1, wide), 1)
    own_ids = jnp.zeros((1, wide), jnp.int32)
    own_column = jnp.zeros((rows, LANES), jnp.int32)
    row_iota = lax.broadcasted_iota(jnp.int32, (rows, LANES), 0)
    for at in range(rows):
        own_ids = jnp.where(lax.rem(wide_row, rows) == at, owned_ref[at], own_ids)
        own_column = jnp.where(row_iota == at, owned_ref[at], own_column)
    ids[0] = own_ids

    def folded(product):
        pieces = [
            product[top : top + 8, left : left + LANES]
            for top in range(0, rows, 8)
            for left in range(0, block, LANES)
        ]
        return jnp.sum(tree(pieces), axis=1, keepdims=True)

    def part_sum(image_value, first):
        tile = jnp.where(lane_tile == SQUARES, folded(image_value * image_value), 0.0)
        tile = jnp.where(lane_tile == SHIFT, folded(diagonal[...]), tile)
        if not first:
            for k in range(STEPS):
                tile = jnp.where(lane_tile == k, folded(known[k] * image_value), tile)
        return jnp.sum(tile, axis=0, keepdims=True)

    def image_copy(buffer, step):
        group, rank = peer(step, 0)
        return pltpu.make_async_remote_copy(
            src_ref=image.at[buffer, 0],
            dst_ref=image.at[buffer, groups - step],
            send_sem=image_send.at[buffer, step],
            recv_sem=image_recv.at[buffer, groups - step],
            device_id=(group, rank),
            device_id_type=MESH,
        )

    def image_wait(buffer, step):
        pltpu.make_async_copy(
            image.at[buffer, step], image.at[buffer, step], image_recv.at[buffer, step]
        ).wait()

    def part_start(buffer):
        def send(group, rank):
            pltpu.make_async_remote_copy(
                src_ref=parts.at[buffer, me],
                dst_ref=parts.at[buffer, me],
                send_sem=part_send.at[buffer],
                recv_sem=part_recv.at[buffer],
                device_id=(group, rank),
                device_id_type=MESH,
            ).start()

        each_other(send)

    def part_wait(buffer, sem):
        others = parts.at[buffer, pl.ds(0, devices - 1)]
        pltpu.make_async_copy(others, others, sem.at[buffer]).wait()

    def id_copy(step):
        group, rank = peer(step, 0)
        return pltpu.make_async_remote_copy(
            src_ref=ids.at[0],
            dst_ref=ids.at[groups - step],
            send_sem=id_send.at[step],
            recv_sem=id_recv.at[groups - step],
            device_id=(group, rank),
            device_id_type=MESH,
        )

    def totals(buffer):
        total = tree([parts[buffer, at] for at in range(devices)]) * (1.0 / entries)
        signed = jnp.where(lane_row < STEPS, -total * total, 0.0)
        signed = jnp.where(lane_row == SQUARES, total, signed)
        square_mean = jnp.sum(signed, axis=1, keepdims=True)
        return total, square_mean

    for s in range(slots):
        row = jnp.where(s < live_ref[0], row_ref[s], -1)
        mask[s] = (own_column == row).astype(F32).astype(BF16)
    known[...] = jnp.zeros_like(known)
    mapped[...] = jnp.zeros_like(mapped)
    column = jnp.full((packed_slots, wide), -1, jnp.int32)
    slot_iota = lax.broadcasted_iota(jnp.int32, (packed_slots, wide), 0)
    for s in range(slots):
        column = jnp.where(slot_iota == s, column_ref[s], column)
    start = start_ref[...]
    image[0, 0] = start

    weight_copy.wait()
    degree = jnp.zeros((rows, block), F32)
    for s in range(slots):
        lhs = jnp.concatenate([mask[s]] * (block // LANES), axis=1)
        degree = degree + lax.dot_general(lhs, weights[s], NT, preferred_element_type=F32)
    diagonal[...] = degree + shift_ref[...]
    parts[0, me] = part_sum(start, True)

    pl.semaphore_wait(barrier, devices - 1)
    for step in range(1, groups):
        image_copy(0, step).start()
    for step in range(1, groups):
        id_copy(step).start()
    part_start(0)

    for step in range(1, groups):
        id_copy(step).wait_send()
    for step in range(1, groups):
        pltpu.make_async_copy(ids.at[step], ids.at[step], id_recv.at[step]).wait()
    known_ids = ids[0]
    for step in range(1, groups):
        known_ids = jnp.where(wide_row // rows == step, ids[step], known_ids)
    gather = (column == known_ids).astype(F32).astype(BF16)

    def reduced(buffer):
        part_wait(buffer, part_recv)
        total, square_mean = totals(buffer)
        tile = jnp.broadcast_to(total, (8, LANES))
        scale = jnp.broadcast_to(lax.rsqrt(square_mean + 1e-06), (8, LANES))
        coefficients = [
            jnp.broadcast_to(tile[:, k : k + 1], (8, LANES)) for k in range(STEPS)
        ]
        shift = jnp.broadcast_to(tile[:, SHIFT : SHIFT + 1], (8, LANES))
        return total, square_mean, coefficients, scale, shift

    def orthogonal(piece_of, history, coefficients, scale):
        lines = []
        for top in range(0, rows, 8):
            line = []
            for left in range(0, block, LANES):
                at = (pl.ds(top, 8), pl.ds(left, LANES))
                terms = [piece_of(top, left)]
                for k in range(STEPS):
                    terms.append(-coefficients[k] * history[(k,) + at])
                line.append(tree(terms) * scale)
            lines.append(jnp.concatenate(line, axis=1))
        return jnp.concatenate(lines, axis=0)

    def vector_of(buffer, coefficients, scale):
        def piece(top, left):
            return image[buffer, 0, pl.ds(top, 8), pl.ds(left, LANES)]

        return orthogonal(piece, known, coefficients, scale)

    def record(it, total, square_mean, shift, alpha, beta):
        here = lane_row == it - 1
        alpha = jnp.where(here, total + shift[:1], alpha)
        beta = jnp.where(here, jnp.sqrt(square_mean), beta)
        return alpha, beta

    def body(it, state):
        alpha, beta = state
        now = lax.rem(it, 2)
        later = 1 - now
        for step in range(1, groups):
            image_wait(now, step)
        high = []
        low = []
        for step in range(groups):
            value = image[now, step]
            top = value.astype(BF16)
            high.append(top)
            low.append((value - top.astype(F32)).astype(BF16))
        both = jnp.concatenate(
            [jnp.concatenate(high, axis=0), jnp.concatenate(low, axis=0)], axis=1
        )
        gathered = jnp.dot(gather, both, preferred_element_type=F32)
        product = jnp.zeros((2 * rows, block), F32)
        for s in range(slots):
            keep = jnp.concatenate([mask[s]] * (block // LANES), axis=1)
            top = jnp.broadcast_to(gathered[s : s + 1, :block], (rows, block)).astype(BF16)
            rest = jnp.broadcast_to(gathered[s : s + 1, block:], (rows, block)).astype(BF16)
            lhs = jnp.concatenate([top * keep, rest * keep], axis=0)
            product = product + lax.dot_general(
                lhs, weights[s], NT, preferred_element_type=F32
            )
        coupling = product[:rows] + product[rows:]

        total, square_mean, coefficients, scale, shift = reduced(now)

        def mapped_piece(top, left):
            at = (pl.ds(top, 8), pl.ds(left, LANES))
            moved = (diagonal[at] - shift) * image[(now, 0) + at]
            return moved - coupling[top : top + 8, left : left + LANES]

        image_value = orthogonal(mapped_piece, mapped, coefficients, scale)
        for step in range(1, groups):
            image_copy(now, step).wait_send()
        image[later, 0] = image_value

        @pl.when(it < STEPS - 1)
        def _():
            for step in range(1, groups):
                image_copy(later, step).start()

        vector = vector_of(now, coefficients, scale)
        known[it] = vector
        part_wait(now, part_send)
        parts[later, me] = part_sum(image_value, False)
        part_start(later)
        mapped[it] = image_value
        basis_ref[it] = vector
        return record(it, total, square_mean, shift, alpha, beta)

    zero = jnp.zeros((1, LANES), F32)
    alpha, beta = lax.fori_loop(0, STEPS, body, (zero, zero))
    last = STEPS % 2
    total, square_mean, coefficients, scale, shift = reduced(last)
    part_wait(last, part_send)
    alpha, beta = record(STEPS, total, square_mean, shift, alpha, beta)
    basis_ref[STEPS] = vector_of(last, coefficients, scale)
    tri_ref[...] = jnp.concatenate([alpha[:, :STEPS], beta[:, :STEPS]], axis=0)


def shards(
    owned_blocks,
    live_count,
    row_block,
    column_block,
    send_list,
    receive_list,
    block_values,
    node_shift,
    start_vector,
):
    rows, block = start_vector.shape
    slots = block_values.shape[0]
    groups = lax.axis_size("grp")
    ranks = lax.axis_size("row")
    devices = groups * ranks
    smem = pl.BlockSpec(memory_space=pltpu.SMEM)
    vmem = pl.BlockSpec(memory_space=pltpu.VMEM)
    dma = pltpu.SemaphoreType.DMA
    return pl.pallas_call(
        functools.partial(kernel, groups, ranks),
        out_shape=(
            jax.ShapeDtypeStruct((STEPS + 1, rows, block), F32),
            jax.ShapeDtypeStruct((2, STEPS), F32),
        ),
        in_specs=[smem, smem, smem, smem, pl.BlockSpec(memory_space=pl.ANY), vmem, vmem],
        out_specs=(vmem, vmem),
        scratch_shapes=[
            pltpu.VMEM((slots, block, block), BF16),
            pltpu.VMEM((slots, rows, LANES), BF16),
            pltpu.VMEM((STEPS, rows, block), F32),
            pltpu.VMEM((STEPS, rows, block), F32),
            pltpu.VMEM((2, groups, rows, block), F32),
            pltpu.VMEM((2, devices, 1, LANES), F32),
            pltpu.VMEM((groups, 1, groups * rows), jnp.int32),
            pltpu.VMEM((rows, block), F32),
            dma,
            dma((2, groups)),
            dma((2, groups)),
            dma((2,)),
            dma((2,)),
            dma((groups,)),
            dma((groups,)),
        ],
        compiler_params=pltpu.CompilerParams(
            collective_id=0, has_side_effects=True, vmem_limit_bytes=48 * 1024 * 1024
        ),
    )(owned_blocks, live_count, row_block, column_block, block_values, node_shift, start_vector)


def solution(mesh):
    return jax.shard_map(
        shards,
        mesh=mesh,
        in_specs=(
            P(("grp", "row")),
            P(("grp", "row")),
            P(("grp", "row")),
            P(("grp", "row")),
            P("grp", "row", None, None),
            P("grp", "row", None, None),
            P(("grp", "row"), None, None),
            P(("grp", "row"), None),
            P(("grp", "row"), None),
        ),
        out_specs=(P(None, ("grp", "row"), None), P()),
        check_vma=False,
    )
```

```python
import functools

import jax
import jax.numpy as jnp
from jax import lax
from jax.experimental import pallas as pl
from jax.experimental.pallas import tpu as pltpu
from jax.sharding import PartitionSpec as P

STEPS = 16
LANES = 128
F32 = jnp.float32
BF16 = jnp.bfloat16
MESH = pl.DeviceIdType.MESH


SQUARES = STEPS + 1
SHIFT = STEPS + 2


def tree(terms):
    while len(terms) > 1:
        pairs = [terms[at] + terms[at + 1] for at in range(0, len(terms) - 1, 2)]
        terms = pairs + terms[len(pairs) * 2 :]
    return terms[0]


def kernel(
    groups,
    ranks,
    owned_ref,
    live_ref,
    row_ref,
    column_ref,
    values_ref,
    shift_ref,
    start_ref,
    basis_ref,
    tri_ref,
    weights,
    mask,
    known,
    mapped,
    image,
    parts,
    ids,
    diagonal,
    weight_sem,
    image_send,
    image_recv,
    part_send,
    part_recv,
    id_send,
    id_recv,
):
    slots, block, _ = values_ref.shape
    rows = shift_ref.shape[0]
    devices = groups * ranks
    entries = float(devices * rows * block)
    my_group = lax.axis_index("grp")
    my_rank = lax.axis_index("row")
    me = my_group * ranks + my_rank
    packed_slots = -(-slots // 8) * 8

    def wrapped(value, size):
        return jnp.where(value >= size, value - size, value)

    if devices <= 64:
        group_at = [wrapped(my_group + step, groups) for step in range(groups)]
        rank_at = [wrapped(my_rank + step, ranks) for step in range(ranks)]

        def peer(group_step, rank_step):
            return group_at[group_step], rank_at[rank_step]

    else:

        def peer(group_step, rank_step):
            return (
                wrapped(my_group + group_step, groups),
                wrapped(my_rank + rank_step, ranks),
            )

    offsets = [(g, r) for r in range(ranks - 1, -1, -1) for g in range(groups - 1, -1, -1)]
    offsets = [pair for pair in offsets if pair != (0, 0)]

    def each_other(action):
        if devices <= 64:
            for group_step, rank_step in offsets:
                action(*peer(group_step, rank_step))
        else:

            def body(at, carry):
                action(*peer(at // ranks, lax.rem(at, ranks)))
                return carry

            lax.fori_loop(1, devices, body, 0)

    weight_copy = pltpu.make_async_copy(values_ref, weights, weight_sem)
    weight_copy.start()

    barrier = pltpu.get_barrier_semaphore()
    each_other(
        lambda g, r: pl.semaphore_signal(barrier, inc=1, device_id=(g, r), device_id_type=MESH)
    )

    lane_row = lax.broadcasted_iota(jnp.int32, (1, LANES), 1)
    lane_tile = lax.broadcasted_iota(jnp.int32, (8, LANES), 1)
    wide = groups * rows
    wide_row = lax.broadcasted_iota(jnp.int32, (1, wide), 1)
    own_ids = jnp.zeros((1, wide), jnp.int32)
    own_column = jnp.zeros((rows, LANES), jnp.int32)
    row_iota = lax.broadcasted_iota(jnp.int32, (rows, LANES), 0)
    for at in range(rows):
        own_ids = jnp.where(lax.rem(wide_row, rows) == at, owned_ref[at], own_ids)
        own_column = jnp.where(row_iota == at, owned_ref[at], own_column)
    ids[0] = own_ids

    def folded(product):
        pieces = [
            product[top : top + 8, left : left + LANES]
            for top in range(0, rows, 8)
            for left in range(0, block, LANES)
        ]
        return jnp.sum(tree(pieces), axis=1, keepdims=True)

    def part_sum(image_value, first):
        tile = jnp.where(lane_tile == SQUARES, folded(image_value * image_value), 0.0)
        tile = jnp.where(lane_tile == SHIFT, folded(diagonal[...]), tile)
        if not first:
            for k in range(STEPS):
                tile = jnp.where(lane_tile == k, folded(known[k] * image_value), tile)
        return jnp.sum(tile, axis=0, keepdims=True)

    def image_copy(buffer, step):
        group, rank = peer(step, 0)
        return pltpu.make_async_remote_copy(
            src_ref=image.at[buffer, 0],
            dst_ref=image.at[buffer, groups - step],
            send_sem=image_send.at[buffer, step],
            recv_sem=image_recv.at[buffer, groups - step],
            device_id=(group, rank),
            device_id_type=MESH,
        )

    def image_wait(buffer, step):
        pltpu.make_async_copy(
            image.at[buffer, step], image.at[buffer, step], image_recv.at[buffer, step]
        ).wait()

    def part_start(buffer):
        def send(group, rank):
            pltpu.make_async_remote_copy(
                src_ref=parts.at[buffer, me],
                dst_ref=parts.at[buffer, me],
                send_sem=part_send.at[buffer],
                recv_sem=part_recv.at[buffer],
                device_id=(group, rank),
                device_id_type=MESH,
            ).start()

        each_other(send)

    def part_wait(buffer, sem):
        others = parts.at[buffer, pl.ds(0, devices - 1)]
        pltpu.make_async_copy(others, others, sem.at[buffer]).wait()

    def id_copy(step):
        group, rank = peer(step, 0)
        return pltpu.make_async_remote_copy(
            src_ref=ids.at[0],
            dst_ref=ids.at[groups - step],
            send_sem=id_send.at[step],
            recv_sem=id_recv.at[groups - step],
            device_id=(group, rank),
            device_id_type=MESH,
        )

    def totals(buffer):
        total = tree([parts[buffer, at] for at in range(devices)]) * (1.0 / entries)
        signed = jnp.where(lane_row < STEPS, -total * total, 0.0)
        signed = jnp.where(lane_row == SQUARES, total, signed)
        square_mean = jnp.sum(signed, axis=1, keepdims=True)
        return total, square_mean

    for s in range(slots):
        row = jnp.where(s < live_ref[0], row_ref[s], -1)
        mask[s] = (own_column == row).astype(F32).astype(BF16)
    known[...] = jnp.zeros_like(known)
    mapped[...] = jnp.zeros_like(mapped)
    column = jnp.full((packed_slots, wide), -1, jnp.int32)
    slot_iota = lax.broadcasted_iota(jnp.int32, (packed_slots, wide), 0)
    for s in range(slots):
        column = jnp.where(slot_iota == s, column_ref[s], column)
    start = start_ref[...]
    image[0, 0] = start

    weight_copy.wait()

    def flip(s, carry):
        weights[s] = weights[s].T
        return carry

    lax.fori_loop(0, slots, flip, 0)
    degree = jnp.zeros((rows, block), F32)
    for s in range(slots):
        lhs = jnp.concatenate([mask[s]] * (block // LANES), axis=1)
        degree = degree + jnp.dot(lhs, weights[s], preferred_element_type=F32)
    diagonal[...] = degree + shift_ref[...]
    parts[0, me] = part_sum(start, True)

    pl.semaphore_wait(barrier, devices - 1)
    for step in range(1, groups):
        image_copy(0, step).start()
    for step in range(1, groups):
        id_copy(step).start()
    part_start(0)

    for step in range(1, groups):
        id_copy(step).wait_send()
    for step in range(1, groups):
        pltpu.make_async_copy(ids.at[step], ids.at[step], id_recv.at[step]).wait()
    known_ids = ids[0]
    for step in range(1, groups):
        known_ids = jnp.where(wide_row // rows == step, ids[step], known_ids)
    gather = (column == known_ids).astype(F32).astype(BF16)

    def reduced(buffer):
        part_wait(buffer, part_recv)
        total, square_mean = totals(buffer)
        tile = jnp.broadcast_to(total, (8, LANES))
        scale = jnp.broadcast_to(lax.rsqrt(square_mean + 1e-06), (8, LANES))
        coefficients = [
            jnp.broadcast_to(tile[:, k : k + 1], (8, LANES)) for k in range(STEPS)
        ]
        shift = jnp.broadcast_to(tile[:, SHIFT : SHIFT + 1], (8, LANES))
        return total, square_mean, coefficients, scale, shift

    def orthogonal(piece_of, history, coefficients, scale):
        lines = []
        for top in range(0, rows, 8):
            line = []
            for left in range(0, block, LANES):
                at = (pl.ds(top, 8), pl.ds(left, LANES))
                terms = [piece_of(top, left)]
                for k in range(STEPS):
                    terms.append(-coefficients[k] * history[(k,) + at])
                line.append(tree(terms) * scale)
            lines.append(jnp.concatenate(line, axis=1))
        return jnp.concatenate(lines, axis=0)

    def vector_of(buffer, coefficients, scale):
        def piece(top, left):
            return image[buffer, 0, pl.ds(top, 8), pl.ds(left, LANES)]

        return orthogonal(piece, known, coefficients, scale)

    def record(it, total, square_mean, shift, alpha, beta):
        here = lane_row == it - 1
        alpha = jnp.where(here, total + shift[:1], alpha)
        beta = jnp.where(here, jnp.sqrt(square_mean), beta)
        return alpha, beta

    def body(it, state):
        alpha, beta = state
        now = lax.rem(it, 2)
        later = 1 - now
        for step in range(1, groups):
            image_wait(now, step)
        high = []
        low = []
        for step in range(groups):
            value = image[now, step]
            top = value.astype(BF16)
            high.append(top)
            low.append((value - top.astype(F32)).astype(BF16))
        both = jnp.concatenate(
            [jnp.concatenate(high, axis=0), jnp.concatenate(low, axis=0)], axis=1
        )
        gathered = jnp.dot(gather, both, preferred_element_type=F32)
        product = jnp.zeros((2 * rows, block), F32)
        for s in range(slots):
            keep = jnp.concatenate([mask[s]] * (block // LANES), axis=1)
            top = jnp.broadcast_to(gathered[s : s + 1, :block], (rows, block)).astype(BF16)
            rest = jnp.broadcast_to(gathered[s : s + 1, block:], (rows, block)).astype(BF16)
            lhs = jnp.concatenate([top * keep, rest * keep], axis=0)
            product = product + jnp.dot(lhs, weights[s], preferred_element_type=F32)
        coupling = product[:rows] + product[rows:]

        total, square_mean, coefficients, scale, shift = reduced(now)

        def mapped_piece(top, left):
            at = (pl.ds(top, 8), pl.ds(left, LANES))
            moved = (diagonal[at] - shift) * image[(now, 0) + at]
            return moved - coupling[top : top + 8, left : left + LANES]

        image_value = orthogonal(mapped_piece, mapped, coefficients, scale)
        for step in range(1, groups):
            image_copy(now, step).wait_send()
        image[later, 0] = image_value

        @pl.when(it < STEPS - 1)
        def _():
            for step in range(1, groups):
                image_copy(later, step).start()

        vector = vector_of(now, coefficients, scale)
        known[it] = vector
        part_wait(now, part_send)
        parts[later, me] = part_sum(image_value, False)
        part_start(later)
        mapped[it] = image_value
        basis_ref[it] = vector
        return record(it, total, square_mean, shift, alpha, beta)

    zero = jnp.zeros((1, LANES), F32)
    alpha, beta = lax.fori_loop(0, STEPS, body, (zero, zero))
    last = STEPS % 2
    total, square_mean, coefficients, scale, shift = reduced(last)
    part_wait(last, part_send)
    alpha, beta = record(STEPS, total, square_mean, shift, alpha, beta)
    basis_ref[STEPS] = vector_of(last, coefficients, scale)
    tri_ref[...] = jnp.concatenate([alpha[:, :STEPS], beta[:, :STEPS]], axis=0)


def shards(
    owned_blocks,
    live_count,
    row_block,
    column_block,
    send_list,
    receive_list,
    block_values,
    node_shift,
    start_vector,
):
    rows, block = start_vector.shape
    slots = block_values.shape[0]
    groups = lax.axis_size("grp")
    ranks = lax.axis_size("row")
    devices = groups * ranks
    smem = pl.BlockSpec(memory_space=pltpu.SMEM)
    vmem = pl.BlockSpec(memory_space=pltpu.VMEM)
    dma = pltpu.SemaphoreType.DMA
    return pl.pallas_call(
        functools.partial(kernel, groups, ranks),
        out_shape=(
            jax.ShapeDtypeStruct((STEPS + 1, rows, block), F32),
            jax.ShapeDtypeStruct((2, STEPS), F32),
        ),
        in_specs=[smem, smem, smem, smem, pl.BlockSpec(memory_space=pl.ANY), vmem, vmem],
        out_specs=(vmem, vmem),
        scratch_shapes=[
            pltpu.VMEM((slots, block, block), BF16),
            pltpu.VMEM((slots, rows, LANES), BF16),
            pltpu.VMEM((STEPS, rows, block), F32),
            pltpu.VMEM((STEPS, rows, block), F32),
            pltpu.VMEM((2, groups, rows, block), F32),
            pltpu.VMEM((2, devices, 1, LANES), F32),
            pltpu.VMEM((groups, 1, groups * rows), jnp.int32),
            pltpu.VMEM((rows, block), F32),
            dma,
            dma((2, groups)),
            dma((2, groups)),
            dma((2,)),
            dma((2,)),
            dma((groups,)),
            dma((groups,)),
        ],
        compiler_params=pltpu.CompilerParams(
            collective_id=0, has_side_effects=True, vmem_limit_bytes=48 * 1024 * 1024
        ),
    )(owned_blocks, live_count, row_block, column_block, block_values, node_shift, start_vector)


def solution(mesh):
    return jax.shard_map(
        shards,
        mesh=mesh,
        in_specs=(
            P(("grp", "row")),
            P(("grp", "row")),
            P(("grp", "row")),
            P(("grp", "row")),
            P("grp", "row", None, None),
            P("grp", "row", None, None),
            P(("grp", "row"), None, None),
            P(("grp", "row"), None),
            P(("grp", "row"), None),
        ),
        out_specs=(P(None, ("grp", "row"), None), P()),
        check_vma=False,
    )
```
